32 devices in a mesh: groups: 2 (over x), row: 16 (over z, y, core).
Axes of the slice: x: 2, y: 2, z: 4, core: 2. Of those that a mesh axis runs over, the one named last changes fastest.
Arguments:
- factor_b: bfloat16 [64, 131072], P(None, ('groups', 'row')), parts along dimension 1, may hold values from -12 to 12
- factor_c: bfloat16 [64, 131072], P(None, ('groups', 'row')), parts along dimension 1, may hold values from -12 to 12
- sample_j: int32 [262144], P(('groups', 'row')), parts along dimension 0, may hold values from 0 to 65535, as said below
- sample_k: int32 [16, 32, 512], P(None, ('groups', 'row')), parts along dimension 1, may hold values from 0 to 65535, as said below
- sample_weight: float32 [262144], P(('groups', 'row')), parts along dimension 0, may hold values from 0.5 to 3.5
- block_values: bfloat16 [32, 16, 4, 4, 128], P(('groups', 'row')), parts along dimension 0, may hold values from -24 to 24
- block_sample: int32 [32, 16, 4, 4], P(('groups', 'row')), parts along dimension 0, may hold values from 0 to 8191
- block_count: int32 [32, 16, 4, 4], P(('groups', 'row')), parts along dimension 0, may hold values from 0 to 128, as said below
Outputs:
- factor_new: bfloat16 [64, 16384], P(None, ('groups', 'row')), parts along dimension 1
- scales: float32 [128], P('groups'), parts along dimension 0
The draws below stay inside these ranges and needn't reach their ends.
There are 2 independent parts, one for each index of `groups`. The reference program is written for one: setup_inputs(seed, part) draws one part's arguments, and reference() takes and returns one part's arrays. A program takes and returns all parts, laid end to end along the dimension named above; each array names one. Nothing has to cross between parts.
Inputs may be any that keep to these rules, and one draw needn't show every extreme that they name: sample_j[s] lies in rows s // 8192 * 4096 to s // 8192 * 4096 + 4095. sample_k[d, e, i] is the third-mode index of sample d * 8192 + e * 512 + i and lies in rows e * 4096 to e * 4096 + 4095. `block_count`: 0 marks an empty slot; slot [p, p, 0, 0] holds 128 for every p.
All inputs are finite; a program needn't handle non-finite values.
Results may differ from the reference program's by a relative error of at most 0.0051.
Values may be sent and summed in bfloat16 or wider, within the bound.
A program may use at most 64 MiB of HBM per device.

```python
import math
import jax
import jax.numpy as jnp
from jax import lax

R = 64
JD = 4096
KD = 4096
S_DEV = 8192
TD = 4
CT = 4
SPN = 512
S = 131072
J = 65536
K = 65536
I = 8192
N_ROW = 16


def factor_draw(key, total_rows):
    key_scale = jax.random.fold_in(key, 11)
    key_own = jax.random.fold_in(key, 12)
    key_spread = jax.random.fold_in(key, 14)
    column_scale = jnp.exp(jax.random.uniform(key_scale, (R, 1), minval=-math.log(1.5), maxval=math.log(1.5)))
    heavy_column = jax.random.randint(key_spread, (1, total_rows), 0, 128, dtype=jnp.int32) == 0
    spread_factor = jnp.where(heavy_column, 5.5, 0.8).astype(jnp.float32)
    own_part = jax.random.normal(key_own, (R, total_rows), dtype=jnp.float32)
    return (jnp.clip(own_part * spread_factor, -8.0, 8.0) * column_scale).astype(jnp.bfloat16)


def draw_factor_b(key, part):
    return factor_draw(jax.random.fold_in(key, 1), J)


def draw_factor_c(key, part):
    return factor_draw(jax.random.fold_in(key, 2), K)


def draw_sample_j(key, part):
    owner_block = jnp.arange(S, dtype=jnp.int32) // S_DEV
    offsets = jax.random.randint(jax.random.fold_in(key, 3), (S,), 0, JD, dtype=jnp.int32)
    return owner_block * JD + offsets


def draw_sample_k(key, part):
    holder = lax.broadcasted_iota(jnp.int32, (N_ROW, N_ROW, SPN), 1)
    offsets = jax.random.randint(jax.random.fold_in(key, 4), (N_ROW, N_ROW, SPN), 0, KD, dtype=jnp.int32)
    return holder * KD + offsets


def draw_sample_weight(key, part):
    device_pos = (jnp.arange(S, dtype=jnp.int32) // S_DEV).astype(jnp.float32)
    lift = jnp.sqrt(1.0 + 2.0 * device_pos / (N_ROW - 1))
    key_base = jax.random.fold_in(key, 5)
    base_weight = jnp.exp(jax.random.uniform(key_base, (S,), minval=-math.log(2.0), maxval=math.log(2.0)))
    return base_weight * lift


def draw_block_values(key, part):
    slot_shape = (N_ROW, N_ROW, TD, CT, 128)
    target = lax.broadcasted_iota(jnp.int32, slot_shape, 1).astype(jnp.float32)
    target_scale = 1.0 + 2.0 * target / (N_ROW - 1)
    key_noise = jax.random.fold_in(key, 6)
    noise_field = jax.random.normal(key_noise, slot_shape, dtype=jnp.float32)
    return (jnp.clip(noise_field, -8.0, 8.0) * target_scale).astype(jnp.bfloat16)


def draw_block_count(key, part):
    slot_shape = (N_ROW, N_ROW, TD, CT)
    source_ids = lax.broadcasted_iota(jnp.int32, slot_shape, 0)
    target_ids = lax.broadcasted_iota(jnp.int32, slot_shape, 1)
    tile_ids = lax.broadcasted_iota(jnp.int32, slot_shape, 2)
    slot_ids = lax.broadcasted_iota(jnp.int32, slot_shape, 3)
    fill_level = jax.random.randint(jax.random.fold_in(key, 7), (N_ROW,), 5, 9, dtype=jnp.int32)
    live_slot = jax.random.randint(jax.random.fold_in(key, 8), slot_shape, 0, 8, dtype=jnp.int32) < fill_level[None, :, None, None]
    most_live = 43 + 85 * source_ids // (N_ROW - 1)
    least_live = most_live // 2
    raw_count = jax.random.randint(jax.random.fold_in(key, 9), slot_shape, 0, 1 << 20, dtype=jnp.int32) % (most_live - least_live) + least_live + 1
    counted = jnp.where(live_slot, raw_count, jnp.zeros_like(raw_count))
    fixed_slot = (source_ids == target_ids) & (tile_ids == 0) & (slot_ids == 0)
    return jnp.where(fixed_slot, jnp.full_like(counted, 128), counted)


def place_ends(drawn, own_key, smallest, top_value):
    place = [jax.random.randint(jax.random.fold_in(own_key, axis), (), 0, length) for axis, length in enumerate(drawn.shape)]
    main_axis = drawn.shape.index(max(drawn.shape))
    beside = place[:main_axis] + [(place[main_axis] + 1) % drawn.shape[main_axis]] + place[main_axis + 1:]
    return drawn.at[tuple(place)].set(smallest).at[tuple(beside)].set(top_value)


def setup_inputs(seed: int = 0, part: int = 0) -> dict:
    key_list = jax.random.split(jax.random.key(seed), 9)
    own_keys = jax.random.split(jax.random.fold_in(key_list[8], part), 9)
    return {
        "factor_b": draw_factor_b(jax.random.fold_in(jax.random.fold_in(key_list[8], part), 71), part),
        "factor_c": draw_factor_c(jax.random.fold_in(jax.random.fold_in(key_list[8], part), 71), part),
        "sample_j": draw_sample_j(jax.random.fold_in(jax.random.fold_in(key_list[8], part), 71), part),
        "sample_k": draw_sample_k(jax.random.fold_in(jax.random.fold_in(key_list[8], part), 71), part),
        "sample_weight": draw_sample_weight(jax.random.fold_in(jax.random.fold_in(key_list[8], part), 71), part),
        "block_values": draw_block_values(jax.random.fold_in(jax.random.fold_in(key_list[8], part), 71), part),
        "block_sample": place_ends(jax.random.randint(own_keys[6], (N_ROW, N_ROW, TD, CT), 0, S_DEV), jax.random.fold_in(own_keys[6], 1), 0, S_DEV - 1).astype(jnp.int32),
        "block_count": draw_block_count(jax.random.fold_in(jax.random.fold_in(key_list[8], part), 71), part),
    }


def reference(factor_b, factor_c, sample_j, sample_k, sample_weight, block_values, block_sample, block_count):
    rank_width = factor_b.shape[0]
    b_columns = jnp.take(factor_b, sample_j, axis=1).astype(jnp.float32)
    c_columns = jnp.take(factor_c, sample_k.reshape(-1), axis=1).astype(jnp.float32)
    sketch = sample_weight[None, :] * b_columns * c_columns
    gram_matrix = jnp.dot(sketch, sketch.T, precision=lax.Precision.HIGHEST)
    live_total = jnp.sum(block_count.astype(jnp.float32))
    ridge = 0.05 * live_total / I
    system = gram_matrix / S + ridge * jnp.eye(rank_width, dtype=jnp.float32)
    lower_factor = jnp.linalg.cholesky(system)
    weighted = (sample_weight[None, :] * sketch).astype(jnp.bfloat16)
    positions = lax.broadcasted_iota(jnp.int32, block_values.shape, 4)
    masked = jnp.where(positions < block_count[..., None], block_values, jnp.zeros_like(block_values))
    owners = lax.broadcasted_iota(jnp.int32, block_sample.shape, 0) * S_DEV + block_sample
    picked = jnp.take(weighted, owners.reshape(-1).astype(jnp.int32), axis=1)
    picked = picked.reshape((rank_width,) + block_sample.shape)
    gathered = jnp.einsum('pqtcr,kpqtc->kqtr', masked.astype(jnp.float32), picked.astype(jnp.float32), precision=lax.Precision.HIGHEST).reshape(rank_width, -1)
    half_solved = lax.linalg.triangular_solve(lower_factor, gathered, left_side=True, lower=True)
    update = lax.linalg.triangular_solve(lower_factor, half_solved, left_side=True, lower=True, transpose_a=True)
    column_sums = lax.optimization_barrier(jnp.sum(update * update, axis=1))
    scales = jnp.sqrt(column_sums / I + 1e-06)
    return ((update / scales[:, None]).astype(jnp.bfloat16), scales)
```

```python
import functools

import jax
import jax.numpy as jnp
from jax import lax
from jax.experimental import pallas as pl
from jax.experimental.pallas import tpu as pltpu
from jax.sharding import PartitionSpec as P

NT = (((1,), (1,)), ((), ()))
TN = (((0,), (0,)), ((), ()))
MESH = pl.DeviceIdType.MESH


def fold_table(table_ref, folded, width):
    rank = table_ref.shape[0]
    for part in range(table_ref.shape[1] // width):
        folded[part * rank : (part + 1) * rank, :] = table_ref[
            :, part * width : (part + 1) * width
        ]


def pick_columns(folded, index, rank):
    width = folded.shape[1]
    count = index.shape[1]
    low = lax.rem(index, width)
    high = lax.div(index, width)
    rows = lax.broadcasted_iota(jnp.int16, (width, count), 0)
    one_hot = jnp.where(rows == low.astype(jnp.int16), jnp.bfloat16(1), jnp.bfloat16(0))
    products = jnp.dot(folded[...], one_hot, preferred_element_type=jnp.float32)
    picked = products[:rank]
    high = jnp.broadcast_to(high, (rank, count))
    for part in range(1, folded.shape[0] // rank):
        picked = jnp.where(high == part, products[part * rank : (part + 1) * rank], picked)
    return picked


def inverse(matrix):
    order = matrix.shape[0]
    lanes = lax.broadcasted_iota(jnp.int32, (1, order), 1)
    rows = lax.broadcasted_iota(jnp.int32, (order, 1), 0)
    for k in range(order):
        row = matrix[k : k + 1, :]
        column = matrix[:, k : k + 1]
        pivot = 1.0 / row[:, k : k + 1]
        scaled = jnp.where(lanes == k, 1.0, row) * pivot
        matrix = jnp.where(
            rows == k, scaled, jnp.where(lanes == k, 0.0, matrix) - column * scaled
        )
    return matrix


def kernel(
    n,
    tiles,
    slots,
    width,
    total_rows,
    total_samples,
    b_ref,
    c_ref,
    j_ref,
    k_ref,
    w_ref,
    values_ref,
    sample_ref,
    count_ref,
    out_ref,
    scales_ref,
    folded_b,
    folded_c,
    c_out,
    c_in,
    b_weighted,
    values_out,
    values_in,
    picks_out,
    picks_in,
    gram_out,
    gram_in,
    sums_out,
    sums_in,
    c_send,
    c_recv,
    values_send,
    values_recv,
    picks_send,
    picks_recv,
    gram_send,
    gram_recv,
    sums_send,
    sums_recv,
):
    me = lax.axis_index("row")
    rank, b_rows = b_ref.shape
    c_rows = c_ref.shape[1]
    half = rank // 2
    per_peer = tiles * slots
    blocks = n * per_peer
    chunk = c_in.shape[2]

    def each_peer(body):
        def step(offset, carry):
            body(lax.rem(me + offset, n))
            return carry

        lax.fori_loop(1, n, step, 0)

    def copy_to(peer, source, target, send, recv):
        return pltpu.make_async_remote_copy(
            src_ref=source,
            dst_ref=target.at[me],
            send_sem=send.at[peer],
            recv_sem=recv.at[me],
            device_id={"row": peer},
            device_id_type=MESH,
        )

    def copy_from(peer, source, target, send, recv):
        return pltpu.make_async_remote_copy(
            src_ref=source,
            dst_ref=target.at[peer],
            send_sem=send.at[peer],
            recv_sem=recv.at[peer],
            device_id={"row": peer},
            device_id_type=MESH,
        )

    barrier = pltpu.get_barrier_semaphore()
    each_peer(
        lambda peer: pl.semaphore_signal(
            barrier, inc=1, device_id={"row": peer}, device_id_type=MESH
        )
    )
    fold_table(c_ref, folded_c, width)
    fold_table(b_ref, folded_b, width)
    lanes = lax.broadcasted_iota(jnp.int32, (blocks, 128), 1)
    live = lanes < count_ref[...]
    masked = jnp.where(live, values_ref[...].astype(jnp.float32), 0.0).astype(jnp.bfloat16)
    values_out[...] = masked.reshape(values_out.shape)
    values_in[me] = values_out[me]
    c_in[me] = pick_columns(folded_c, k_ref[me] - me * c_rows, rank).astype(jnp.bfloat16)
    pl.semaphore_wait(barrier, n - 1)

    def send_c(peer):
        c_out[peer] = pick_columns(folded_c, k_ref[peer] - me * c_rows, rank).astype(
            jnp.bfloat16
        )
        copy_to(peer, c_out.at[peer], c_in, c_send, c_recv).start()

    each_peer(send_c)
    each_peer(
        lambda peer: copy_to(
            peer, values_out.at[peer], values_in, values_send, values_recv
        ).start()
    )

    def pick_b(part, carry):
        picked = pick_columns(folded_b, j_ref[part] - me * b_rows, rank)
        b_weighted[part] = w_ref[part] * picked
        return carry

    lax.fori_loop(0, n, pick_b, 0)

    columns = lax.broadcasted_iota(jnp.int32, (blocks, chunk), 1)

    def add_chunk(part, carry):
        gram, picks = carry
        weights = w_ref[part]
        sketch = b_weighted[part] * c_in[part].astype(jnp.float32)
        top = sketch.astype(jnp.bfloat16)
        rest = (sketch - top.astype(jnp.float32)).astype(jnp.bfloat16)
        both = jnp.concatenate([top, rest], axis=0)
        gram = gram + lax.dot_general(both, both, NT, preferred_element_type=jnp.float32)
        weighted = (weights * sketch).astype(jnp.bfloat16)
        chosen = columns == sample_ref[...] - part * chunk
        chosen = jnp.where(chosen, 1.0, 0.0).astype(jnp.bfloat16)
        picks = picks + lax.dot_general(
            chosen, weighted, NT, preferred_element_type=jnp.float32
        )
        return gram, picks

    def add_peer(offset, carry):
        part = lax.rem(me + n - offset, n)
        copy_from(part, c_out.at[part], c_in, c_send, c_recv).wait_recv()
        return add_chunk(part, carry)

    carry = (
        jnp.zeros((2 * rank, 2 * rank), jnp.float32),
        jnp.zeros((blocks, rank), jnp.float32),
    )
    carry = add_chunk(me, carry)
    gram, picks = lax.fori_loop(1, n, add_peer, carry)

    gram = gram[:rank, :rank] + gram[:rank, rank:] + gram[rank:, :rank] + gram[rank:, rank:]
    live_local = jnp.sum(count_ref[...].astype(jnp.float32), axis=0, keepdims=True)
    gram_out[:half, :] = jnp.concatenate([gram[:half], gram[half:]], axis=1)
    gram_out[half:, :] = jnp.broadcast_to(live_local, (8, 2 * rank))
    gram_in[me] = gram_out[...]
    picks = jnp.concatenate([picks, jnp.zeros_like(picks)], axis=1).astype(jnp.bfloat16)
    picks_out[...] = picks.reshape(picks_out.shape)
    picks_in[me] = picks_out[me]

    def send_sums(peer):
        copy_to(peer, gram_out, gram_in, gram_send, gram_recv).start()
        copy_to(peer, picks_out.at[peer], picks_in, picks_send, picks_recv).start()

    each_peer(send_sums)

    def receive_sums(peer):
        copy_from(peer, gram_out, gram_in, gram_send, gram_recv).wait_recv()

    each_peer(receive_sums)
    total = lax.fori_loop(
        1, n, lambda part, carry: carry + gram_in[part], gram_in[0]
    )
    ridge = 0.05 * total[half : half + 1, :rank] / total_rows
    gram = jnp.concatenate([total[:half, :rank], total[:half, rank:]], axis=0)
    gram_rows = lax.broadcasted_iota(jnp.int32, (rank, rank), 0)
    diagonal = gram_rows == lax.broadcasted_iota(jnp.int32, (rank, rank), 1)
    system = gram / total_samples + jnp.where(diagonal, ridge, 0.0)
    inverted = inverse(system)

    def receive_blocks(peer):
        copy_from(
            peer, values_out.at[peer], values_in, values_send, values_recv
        ).wait_recv()
        copy_from(peer, picks_out.at[peer], picks_in, picks_send, picks_recv).wait_recv()

    each_peer(receive_blocks)
    arrived = values_in[...].reshape(blocks, 128).astype(jnp.float32)
    block_rows = lax.broadcasted_iota(jnp.int32, (blocks, 128), 0)
    tile_of = lax.rem(lax.div(block_rows, slots), tiles)
    spread = jnp.concatenate(
        [jnp.where(tile_of == tile, arrived, 0.0) for tile in range(tiles)], axis=1
    ).astype(jnp.bfloat16)
    gathered = lax.dot_general(
        picks_in[...].reshape(blocks, 2 * rank), spread, TN, preferred_element_type=jnp.float32
    )[:rank]
    update = jnp.dot(
        inverted,
        gathered,
        precision=lax.Precision.HIGHEST,
        preferred_element_type=jnp.float32,
    )
    squares = jnp.sum(update * update, axis=1, keepdims=True)
    squares = jnp.sum(jnp.where(diagonal, squares, 0.0), axis=0, keepdims=True)
    squares = jnp.concatenate([squares, jnp.zeros_like(squares)], axis=1)
    sums_out[...] = jnp.broadcast_to(squares, sums_out.shape)
    sums_in[me] = sums_out[...]
    each_peer(
        lambda peer: copy_to(peer, sums_out, sums_in, sums_send, sums_recv).start()
    )
    each_peer(
        lambda peer: copy_from(peer, sums_out, sums_in, sums_send, sums_recv).wait_recv()
    )
    sums = lax.fori_loop(1, n, lambda part, carry: carry + sums_in[part], sums_in[0])
    scales = jnp.sqrt(sums[:1, :rank] / total_rows + 1e-06)
    scales_ref[...] = scales
    scale_column = jnp.sum(jnp.where(diagonal, scales, 0.0), axis=1, keepdims=True)
    out_ref[...] = (update / scale_column).astype(out_ref.dtype)

    def finish(peer):
        copy_to(peer, c_out.at[peer], c_in, c_send, c_recv).wait_send()
        copy_to(peer, values_out.at[peer], values_in, values_send, values_recv).wait_send()
        copy_to(peer, gram_out, gram_in, gram_send, gram_recv).wait_send()
        copy_to(peer, picks_out.at[peer], picks_in, picks_send, picks_recv).wait_send()
        copy_to(peer, sums_out, sums_in, sums_send, sums_recv).wait_send()

    each_peer(finish)


def shards(
    factor_b, factor_c, sample_j, sample_k, sample_weight, block_values, block_sample, block_count
):
    rank, b_rows = factor_b.shape
    n, _, chunk = sample_k.shape
    _, _, tiles, slots, tile_rows = block_values.shape
    samples = sample_j.shape[0]
    per_peer = tiles * slots
    blocks = n * per_peer
    width = 512
    bf16, f32 = jnp.bfloat16, jnp.float32
    vmem = pl.BlockSpec(memory_space=pltpu.VMEM)
    factor_new, scales = pl.pallas_call(
        functools.partial(
            kernel, n, tiles, slots, width, tiles * tile_rows * n, samples * n
        ),
        out_shape=(
            jax.ShapeDtypeStruct((rank, tiles * tile_rows), bf16),
            jax.ShapeDtypeStruct((1, rank), f32),
        ),
        in_specs=[vmem] * 8,
        out_specs=(vmem, vmem),
        scratch_shapes=[
            pltpu.VMEM((b_rows // width * rank, width), bf16),
            pltpu.VMEM((factor_c.shape[1] // width * rank, width), bf16),
            pltpu.VMEM((n, rank, chunk), bf16),
            pltpu.VMEM((n, rank, chunk), bf16),
            pltpu.VMEM((n, rank, chunk), f32),
            pltpu.VMEM((n, per_peer, tile_rows), bf16),
            pltpu.VMEM((n, per_peer, tile_rows), bf16),
            pltpu.VMEM((n, per_peer, 2 * rank), bf16),
            pltpu.VMEM((n, per_peer, 2 * rank), bf16),
            pltpu.VMEM((rank // 2 + 8, 2 * rank), f32),
            pltpu.VMEM((n, rank // 2 + 8, 2 * rank), f32),
            pltpu.VMEM((8, 2 * rank), f32),
            pltpu.VMEM((n, 8, 2 * rank), f32),
        ]
        + [pltpu.SemaphoreType.DMA((n,))] * 10,
        compiler_params=pltpu.CompilerParams(collective_id=0, has_side_effects=True),
    )(
        factor_b,
        factor_c,
        sample_j.reshape(n, 1, chunk),
        sample_k,
        sample_weight.reshape(n, 1, chunk),
        block_values.reshape(blocks, tile_rows),
        block_sample.reshape(blocks, 1),
        block_count.reshape(blocks, 1),
    )
    return factor_new, scales.reshape(rank)


def solution(mesh):
    in_specs = (
        P(None, ("groups", "row")),
        P(None, ("groups", "row")),
        P(("groups", "row")),
        P(None, ("groups", "row"), None),
        P(("groups", "row")),
        P(("groups", "row"), None, None, None, None),
        P(("groups", "row"), None, None, None),
        P(("groups", "row"), None, None, None),
    )
    out_specs = (P(None, ("groups", "row")), P("groups"))
    return jax.shard_map(shards, mesh=mesh, in_specs=in_specs, out_specs=out_specs, check_vma=False)
```

```python
import functools

import jax
import jax.numpy as jnp
from jax import lax
from jax.experimental import pallas as pl
from jax.experimental.pallas import tpu as pltpu
from jax.sharding import PartitionSpec as P

NT = (((1,), (1,)), ((), ()))
TN = (((0,), (0,)), ((), ()))
MESH = pl.DeviceIdType.MESH


def fold_table(table_ref, folded, width):
    rank = table_ref.shape[0]
    for part in range(table_ref.shape[1] // width):
        folded[part * rank : (part + 1) * rank, :] = table_ref[
            :, part * width : (part + 1) * width
        ]


def pick_columns(folded, index, rank):
    width = folded.shape[1]
    count = index.shape[1]
    low = lax.rem(index, width)
    high = lax.div(index, width)
    rows = lax.broadcasted_iota(jnp.int16, (width, count), 0)
    one_hot = jnp.where(rows == low.astype(jnp.int16), jnp.bfloat16(1), jnp.bfloat16(0))
    products = jnp.dot(folded[...], one_hot, preferred_element_type=jnp.float32)
    picked = products[:rank]
    high = jnp.broadcast_to(high, (rank, count))
    for part in range(1, folded.shape[0] // rank):
        picked = jnp.where(high == part, products[part * rank : (part + 1) * rank], picked)
    return picked


def partner(me, mask, n):
    other, bit = 0, 1
    while bit < n:
        other = other + bit * lax.rem(lax.div(me, bit) + lax.div(mask, bit), 2)
        bit *= 2
    return other


def block_column(table_ref):
    table = jnp.concatenate([table_ref[tile] for tile in range(table_ref.shape[0])], axis=0)
    return jnp.concatenate(
        [table[:, peer : peer + 1] for peer in range(table.shape[1])], axis=0
    )


def inverse(matrix):
    order = matrix.shape[0]
    lanes = lax.broadcasted_iota(jnp.int32, (1, order), 1)
    rows = lax.broadcasted_iota(jnp.int32, (order, 1), 0)
    for k in range(order):
        row = matrix[k : k + 1, :]
        column = matrix[:, k : k + 1]
        pivot = 1.0 / row[:, k : k + 1]
        scaled = jnp.where(lanes == k, 1.0, row) * pivot
        matrix = jnp.where(
            rows == k, scaled, jnp.where(lanes == k, 0.0, matrix) - column * scaled
        )
    return matrix


def kernel(
    n,
    tiles,
    slots,
    width,
    total_rows,
    total_samples,
    b_ref,
    c_ref,
    j_ref,
    k_ref,
    w_ref,
    values_ref,
    sample_ref,
    count_ref,
    out_ref,
    scales_ref,
    folded_b,
    folded_c,
    c_out,
    c_in,
    b_weighted,
    values_out,
    values_in,
    picks_out,
    picks_in,
    gram_out,
    gram_in,
    share_out,
    share_in,
    sample_column,
    sums_out,
    sums_in,
    c_send,
    c_recv,
    values_send,
    values_recv,
    picks_send,
    picks_recv,
    gram_send,
    gram_recv,
    share_send,
    share_recv,
    sums_send,
    sums_recv,
):
    me = lax.axis_index("row")
    rank, b_rows = b_ref.shape
    c_rows = c_ref.shape[1]
    share = rank // n
    per_peer = tiles * slots
    blocks = n * per_peer
    chunk = c_in.shape[2]

    def each_peer(body):
        def step(turn, carry):
            body(partner(me, n - turn, n))
            return carry

        lax.fori_loop(1, n, step, 0)

    def copy_to(peer, source, target, send, recv):
        return pltpu.make_async_remote_copy(
            src_ref=source,
            dst_ref=target.at[me],
            send_sem=send.at[peer],
            recv_sem=recv.at[me],
            device_id={"row": peer},
            device_id_type=MESH,
        )

    def copy_from(peer, source, target, send, recv):
        return pltpu.make_async_remote_copy(
            src_ref=source,
            dst_ref=target.at[peer],
            send_sem=send.at[peer],
            recv_sem=recv.at[peer],
            device_id={"row": peer},
            device_id_type=MESH,
        )

    barrier = pltpu.get_barrier_semaphore()
    each_peer(
        lambda peer: pl.semaphore_signal(
            barrier, inc=1, device_id={"row": peer}, device_id_type=MESH
        )
    )
    fold_table(c_ref, folded_c, width)
    fold_table(b_ref, folded_b, width)
    lanes = lax.broadcasted_iota(jnp.int32, (blocks, 128), 1)
    counts = block_column(count_ref)
    live = lanes < counts
    masked = jnp.where(live, values_ref[...].astype(jnp.float32), 0.0).astype(jnp.bfloat16)
    values_out[...] = masked.reshape(values_out.shape)
    values_in[me] = values_out[me]
    c_in[me] = pick_columns(folded_c, k_ref[me] - me * c_rows, rank).astype(jnp.bfloat16)
    pl.semaphore_wait(barrier, n - 1)

    def send_c(peer):
        c_out[peer] = pick_columns(folded_c, k_ref[peer] - me * c_rows, rank).astype(
            jnp.bfloat16
        )
        copy_to(peer, c_out.at[peer], c_in, c_send, c_recv).start()

    each_peer(send_c)
    each_peer(
        lambda peer: copy_to(
            peer, values_out.at[peer], values_in, values_send, values_recv
        ).start()
    )

    def pick_b(part, carry):
        picked = pick_columns(folded_b, j_ref[part] - me * b_rows, rank)
        b_weighted[part] = w_ref[part] * picked
        return carry

    lax.fori_loop(0, n, pick_b, 0)

    columns = lax.broadcasted_iota(jnp.int32, (blocks, chunk), 1)
    sample_column[...] = block_column(sample_ref)
    counts = block_column(count_ref)

    def add_chunk(part, carry):
        gram, picks = carry
        weights = w_ref[part]
        sketch = b_weighted[part] * c_in[part].astype(jnp.float32)
        top = sketch.astype(jnp.bfloat16)
        rest = (sketch - top.astype(jnp.float32)).astype(jnp.bfloat16)
        both = jnp.concatenate([top, rest], axis=0)
        gram = gram + lax.dot_general(both, both, NT, preferred_element_type=jnp.float32)
        weighted = (weights * sketch).astype(jnp.bfloat16)
        chosen = columns == sample_column[...] - part * chunk
        chosen = jnp.where(chosen, 1.0, 0.0).astype(jnp.bfloat16)
        picks = picks + lax.dot_general(
            chosen, weighted, NT, preferred_element_type=jnp.float32
        )
        return gram, picks

    def add_peer(turn, carry):
        part = partner(me, n - turn, n)
        copy_from(part, c_out.at[part], c_in, c_send, c_recv).wait_recv()
        return add_chunk(part, carry)

    carry = (
        jnp.zeros((2 * rank, 2 * rank), jnp.float32),
        jnp.zeros((blocks, rank), jnp.float32),
    )
    carry = add_chunk(me, carry)
    gram, picks = lax.fori_loop(1, n, add_peer, carry)

    gram = gram[:rank, :rank] + gram[:rank, rank:] + gram[rank:, :rank] + gram[rank:, rank:]
    live_local = jnp.sum(counts.astype(jnp.float32), axis=0, keepdims=True)
    gram = jnp.concatenate([gram, jnp.broadcast_to(live_local, gram.shape)], axis=1)
    gram_out[...] = jnp.zeros_like(gram_out)
    for part in range(n):
        gram_out[part, :share, :] = gram[part * share : (part + 1) * share]
    gram_in[me] = gram_out[me]
    picks = jnp.concatenate([picks, jnp.zeros_like(picks)], axis=1).astype(jnp.bfloat16)
    picks_out[...] = picks.reshape(picks_out.shape)
    picks_in[me] = picks_out[me]

    def send_sums(peer):
        copy_to(peer, gram_out.at[peer], gram_in, gram_send, gram_recv).start()
        copy_to(peer, picks_out.at[peer], picks_in, picks_send, picks_recv).start()

    each_peer(send_sums)

    def receive_sums(peer):
        copy_from(peer, gram_out.at[peer], gram_in, gram_send, gram_recv).wait_recv()

    each_peer(receive_sums)
    share_out[...] = lax.fori_loop(
        1, n, lambda part, carry: carry + gram_in[part], gram_in[0]
    )
    share_in[me] = share_out[...]
    each_peer(
        lambda peer: copy_to(peer, share_out, share_in, share_send, share_recv).start()
    )

    def receive_blocks(peer):
        copy_from(
            peer, values_out.at[peer], values_in, values_send, values_recv
        ).wait_recv()
        copy_from(peer, picks_out.at[peer], picks_in, picks_send, picks_recv).wait_recv()

    each_peer(receive_blocks)
    arrived = values_in[...].reshape(blocks, 128).astype(jnp.float32)
    block_rows = lax.broadcasted_iota(jnp.int32, (blocks, 128), 0)
    tile_of = lax.rem(lax.div(block_rows, slots), tiles)
    spread = jnp.concatenate(
        [jnp.where(tile_of == tile, arrived, 0.0) for tile in range(tiles)], axis=1
    ).astype(jnp.bfloat16)
    gathered = lax.dot_general(
        picks_in[...].reshape(blocks, 2 * rank), spread, TN, preferred_element_type=jnp.float32
    )[:rank]
    each_peer(
        lambda peer: copy_from(peer, share_out, share_in, share_send, share_recv).wait_recv()
    )
    total = jnp.concatenate([share_in[part][:share] for part in range(n)], axis=0)
    ridge = 0.05 * total[:1, rank:] / total_rows
    gram_rows = lax.broadcasted_iota(jnp.int32, (rank, rank), 0)
    diagonal = gram_rows == lax.broadcasted_iota(jnp.int32, (rank, rank), 1)
    system = total[:, :rank] / total_samples + jnp.where(diagonal, ridge, 0.0)
    inverted = inverse(system)
    update = jnp.dot(
        inverted,
        gathered,
        precision=lax.Precision.HIGHEST,
        preferred_element_type=jnp.float32,
    )
    squares = jnp.sum(update * update, axis=1, keepdims=True)
    squares = jnp.sum(jnp.where(diagonal, squares, 0.0), axis=0, keepdims=True)
    squares = jnp.concatenate([squares, jnp.zeros_like(squares)], axis=1)
    sums_out[...] = jnp.broadcast_to(squares, sums_out.shape)
    sums_in[me] = sums_out[...]
    each_peer(
        lambda peer: copy_to(peer, sums_out, sums_in, sums_send, sums_recv).start()
    )
    each_peer(
        lambda peer: copy_from(peer, sums_out, sums_in, sums_send, sums_recv).wait_recv()
    )
    sums = lax.fori_loop(1, n, lambda part, carry: carry + sums_in[part], sums_in[0])
    scales = jnp.sqrt(sums[:1, :rank] / total_rows + 1e-06)
    scales_ref[...] = scales
    scale_column = jnp.sum(jnp.where(diagonal, scales, 0.0), axis=1, keepdims=True)
    out_ref[...] = (update / scale_column).astype(out_ref.dtype)

    def finish(peer):
        copy_to(peer, c_out.at[peer], c_in, c_send, c_recv).wait_send()
        copy_to(peer, values_out.at[peer], values_in, values_send, values_recv).wait_send()
        copy_to(peer, gram_out.at[peer], gram_in, gram_send, gram_recv).wait_send()
        copy_to(peer, share_out, share_in, share_send, share_recv).wait_send()
        copy_to(peer, picks_out.at[peer], picks_in, picks_send, picks_recv).wait_send()
        copy_to(peer, sums_out, sums_in, sums_send, sums_recv).wait_send()

    each_peer(finish)


def shards(
    factor_b, factor_c, sample_j, sample_k, sample_weight, block_values, block_sample, block_count
):
    rank, b_rows = factor_b.shape
    n, _, chunk = sample_k.shape
    _, _, tiles, slots, tile_rows = block_values.shape
    samples = sample_j.shape[0]
    per_peer = tiles * slots
    blocks = n * per_peer
    width = 512
    bf16, f32 = jnp.bfloat16, jnp.float32
    vmem = pl.BlockSpec(memory_space=pltpu.VMEM)
    factor_new, scales = pl.pallas_call(
        functools.partial(
            kernel, n, tiles, slots, width, tiles * tile_rows * n, samples * n
        ),
        out_shape=(
            jax.ShapeDtypeStruct((rank, tiles * tile_rows), bf16),
            jax.ShapeDtypeStruct((1, rank), f32),
        ),
        in_specs=[vmem] * 8,
        out_specs=(vmem, vmem),
        scratch_shapes=[
            pltpu.VMEM((b_rows // width * rank, width), bf16),
            pltpu.VMEM((factor_c.shape[1] // width * rank, width), bf16),
            pltpu.VMEM((n, rank, chunk), bf16),
            pltpu.VMEM((n, rank, chunk), bf16),
            pltpu.VMEM((n, rank, chunk), f32),
            pltpu.VMEM((n, per_peer, tile_rows), bf16),
            pltpu.VMEM((n, per_peer, tile_rows), bf16),
            pltpu.VMEM((n, per_peer, 2 * rank), bf16),
            pltpu.VMEM((n, per_peer, 2 * rank), bf16),
            pltpu.VMEM((n, 8, 2 * rank), f32),
            pltpu.VMEM((n, 8, 2 * rank), f32),
            pltpu.VMEM((8, 2 * rank), f32),
            pltpu.VMEM((n, 8, 2 * rank), f32),
            pltpu.VMEM((blocks, 1), jnp.int32),
            pltpu.VMEM((8, 2 * rank), f32),
            pltpu.VMEM((n, 8, 2 * rank), f32),
        ]
        + [pltpu.SemaphoreType.DMA((n,))] * 12,
        compiler_params=pltpu.CompilerParams(collective_id=0, has_side_effects=True),
    )(
        factor_b,
        factor_c,
        sample_j.reshape(n, 1, chunk),
        sample_k,
        sample_weight.reshape(n, 1, chunk),
        block_values.reshape(blocks, tile_rows),
        block_sample[0].transpose(1, 2, 0),
        block_count[0].transpose(1, 2, 0),
    )
    return factor_new, scales.reshape(rank)


def solution(mesh):
    in_specs = (
        P(None, ("groups", "row")),
        P(None, ("groups", "row")),
        P(("groups", "row")),
        P(None, ("groups", "row"), None),
        P(("groups", "row")),
        P(("groups", "row"), None, None, None, None),
        P(("groups", "row"), None, None, None),
        P(("groups", "row"), None, None, None),
    )
    out_specs = (P(None, ("groups", "row")), P("groups"))
    return jax.shard_map(shards, mesh=mesh, in_specs=in_specs, out_specs=out_specs, check_vma=False)
```
